32 devices in a mesh: batch: 4 (over z), cols: 8 (over y, x, core).
Axes of the slice: x: 2, y: 2, z: 4, core: 2. Of those that a mesh axis runs over, the one named last changes fastest.
Arguments:
- grad_up: float32 [4, 1024, 4096], P('batch', None, 'cols'), may hold values from -0.875 to 0.875
- grad_down: float32 [4, 4096, 1024], P('batch', 'cols'), may hold values from -0.875 to 0.875
- grad_query: float32 [4, 1024, 1024], P('batch', None, 'cols'), may hold values from -0.875 to 0.875
- grad_key: float32 [4, 1024, 1024], P('batch', None, 'cols'), may hold values from -0.875 to 0.875
- grad_value: float32 [4, 1024, 1024], P('batch', None, 'cols'), may hold values from -0.875 to 0.875
- grad_mixed: float32 [4, 1024, 1024], P('batch', 'cols'), may hold values from -0.875 to 0.875
- grad_norm: float32 [4, 1024], P('batch'), may hold values from -8 to 8
- grad_bias: float32 [4, 1024], P('batch'), may hold values from -8 to 8
- weight_up: float32 [1024, 4096], P('batch', 'cols'), may hold values from -0.25 to 0.25
- weight_down: float32 [4096, 1024], P('cols', 'batch'), may hold values from -0.125 to 0.125
- weight_query: float32 [1024, 1024], P('batch', 'cols'), may hold values from -0.25 to 0.25
- weight_key: float32 [1024, 1024], P('batch', 'cols'), may hold values from -0.25 to 0.25
- weight_value: float32 [1024, 1024], P('batch', 'cols'), may hold values from -0.25 to 0.25
- weight_mixed: float32 [1024, 1024], P('cols', 'batch'), may hold values from -0.25 to 0.25
- weight_norm: float32 [1024], P('batch'), may hold values from 0.25 to 1.75
- weight_bias: float32 [1024], P('batch'), may hold values from -3 to 3
- moment_up: float32 [1024, 4096], P('batch', 'cols'), may hold values from -0.1875 to 0.1875
- moment_down: float32 [4096, 1024], P('cols', 'batch'), may hold values from -0.09375 to 0.09375
- moment_query: float32 [1024, 1024], P('batch', 'cols'), may hold values from -0.1875 to 0.1875
- moment_key: float32 [1024, 1024], P('batch', 'cols'), may hold values from -0.1875 to 0.1875
- moment_value: float32 [1024, 1024], P('batch', 'cols'), may hold values from -0.1875 to 0.1875
- moment_mixed: float32 [1024, 1024], P('cols', 'batch'), may hold values from -0.1875 to 0.1875
- moment_norm: float32 [1024], P('batch'), may hold values from -1.75 to 1.75
- moment_bias: float32 [1024], P('batch'), may hold values from -1.75 to 1.75
Outputs:
- copy_up: bfloat16 [1024, 4096], P(None, 'cols')
- copy_down: bfloat16 [4096, 1024], P('cols')
- copy_query: bfloat16 [1024, 1024], P(None, 'cols')
- copy_key: bfloat16 [1024, 1024], P(None, 'cols')
- copy_value: bfloat16 [1024, 1024], P(None, 'cols')
- copy_mixed: bfloat16 [1024, 1024], P('cols')
- copy_norm: bfloat16 [1024], replicated
- copy_bias: bfloat16 [1024], replicated
- new_up: float32 [1024, 4096], P('batch', 'cols')
- new_down: float32 [4096, 1024], P('cols', 'batch')
- new_query: float32 [1024, 1024], P('batch', 'cols')
- new_key: float32 [1024, 1024], P('batch', 'cols')
- new_value: float32 [1024, 1024], P('batch', 'cols')
- new_mixed: float32 [1024, 1024], P('cols', 'batch')
- new_norm: float32 [1024], P('batch')
- new_bias: float32 [1024], P('batch')
- state_new_up: float32 [1024, 4096], P('batch', 'cols')
- state_new_down: float32 [4096, 1024], P('cols', 'batch')
- state_new_query: float32 [1024, 1024], P('batch', 'cols')
- state_new_key: float32 [1024, 1024], P('batch', 'cols')
- state_new_value: float32 [1024, 1024], P('batch', 'cols')
- state_new_mixed: float32 [1024, 1024], P('cols', 'batch')
- state_new_norm: float32 [1024], P('batch')
- state_new_bias: float32 [1024], P('batch')
The draws below stay inside these ranges and needn't reach their ends.
All inputs are finite; a program needn't handle non-finite values.
Results may differ from the reference program's by a relative error of at most 0.001.
Values may be sent and summed in bfloat16 or wider, within the bound.
A program may use at most 64 MiB of HBM per device.

```python
import jax
import jax.numpy as jnp
from jax import lax

WIDTH = 1024
INNER = 4096
ATTN = 1024
REPLICAS = 4


def raised(entries, own_key, source, target, shards_of, factor):
    def block_of(axis_at):
        return (jnp.arange(entries.shape[axis_at]) // (entries.shape[axis_at] // shards_of)).reshape((-1,) + (1,) * (entries.ndim - 1 - axis_at))

    one_side = jax.random.permutation(own_key, shards_of)[block_of(target)]
    far = (block_of(target) + shards_of // 2) % shards_of
    return jnp.where((block_of(source) == one_side) | (block_of(source) == far), factor * entries, entries)


def block_scale(stream_key, dims, shards, smallest, largest):
    factor_of = 1.0
    for dim, parts in shards:
        steps = jax.random.uniform(jax.random.fold_in(jax.random.fold_in(stream_key, 6), dim), (parts,), jnp.float32, smallest / len(shards), largest / len(shards))
        factor_of = factor_of * jnp.repeat(jnp.exp(steps), dims[dim] // parts).reshape((-1,) + (1,) * (len(dims) - 1 - dim))
    return factor_of


def centred(rng, shape, width, bound, shards=(), dtype=jnp.bfloat16):
    result = jax.random.normal(rng, shape, jnp.float32) * width
    if len(shards) > 0:
        result = block_scale(rng, shape, shards, -0.22, 0.18) * result
    return jnp.clip(result, min=-bound, max=bound).astype(dtype)


def heavy_noise(stream_key, extent, width, bound, shards, heavy, kind=jnp.bfloat16):
    drawn = width * jax.random.normal(stream_key, extent, jnp.float32)
    if shards:
        drawn = drawn * block_scale(stream_key, extent, shards, -0.22, 0.18)
    return jnp.clip(raised(drawn, jax.random.fold_in(stream_key, 3), *heavy), -bound, bound).astype(kind)


def setup_inputs(seed: int = 0) -> dict:
    splits = jax.random.split(jax.random.key(seed), 25)
    grad_up = heavy_noise(splits[0], (REPLICAS, WIDTH, INNER), 0.1, 0.875, ((0, 4), (2, 8)), (0, 1, 4, 2.0), jnp.float32)
    grad_down = heavy_noise(splits[1], (REPLICAS, INNER, WIDTH), 0.1, 0.875, ((0, 4), (1, 8)), (0, 2, 4, 2.0), jnp.float32)
    grad_query = heavy_noise(splits[2], (REPLICAS, WIDTH, ATTN), 0.1, 0.875, ((0, 4), (2, 8)), (0, 1, 4, 2.0), jnp.float32)
    grad_key = heavy_noise(splits[3], (REPLICAS, WIDTH, ATTN), 0.1, 0.875, ((0, 4), (2, 8)), (0, 1, 4, 2.0), jnp.float32)
    grad_value = heavy_noise(splits[4], (REPLICAS, WIDTH, ATTN), 0.1, 0.875, ((0, 4), (2, 8)), (0, 1, 4, 2.0), jnp.float32)
    grad_mixed = heavy_noise(splits[5], (REPLICAS, ATTN, WIDTH), 0.1, 0.875, ((0, 4), (1, 8)), (0, 2, 4, 2.0), jnp.float32)
    grad_norm = heavy_noise(splits[6], (REPLICAS, WIDTH), 1.0, 8.0, ((0, 4),), (0, 1, 4, 2.0), jnp.float32)
    grad_bias = heavy_noise(splits[7], (REPLICAS, WIDTH), 1.0, 8.0, ((0, 4),), (0, 1, 4, 2.0), jnp.float32)
    weight_up = heavy_noise(splits[8], (WIDTH, INNER), WIDTH ** -0.5, 0.25, ((0, 4), (1, 8)), (1, 0, 8, 2.0), jnp.float32)
    weight_down = heavy_noise(splits[9], (INNER, WIDTH), INNER ** -0.5, 0.125, ((0, 8), (1, 4)), (0, 1, 8, 2.0), jnp.float32)
    weight_query = heavy_noise(splits[10], (WIDTH, ATTN), WIDTH ** -0.5, 0.25, ((0, 4), (1, 8)), (1, 0, 8, 2.0), jnp.float32)
    weight_key = heavy_noise(splits[11], (WIDTH, ATTN), WIDTH ** -0.5, 0.25, ((0, 4), (1, 8)), (1, 0, 8, 2.0), jnp.float32)
    weight_value = heavy_noise(splits[12], (WIDTH, ATTN), WIDTH ** -0.5, 0.25, ((0, 4), (1, 8)), (1, 0, 8, 2.0), jnp.float32)
    weight_mixed = heavy_noise(splits[13], (ATTN, WIDTH), ATTN ** -0.5, 0.25, ((0, 8), (1, 4)), (0, 1, 8, 2.0), jnp.float32)
    weight_norm = jnp.clip(1.0 + 0.15 * jax.random.normal(splits[14], (WIDTH,), jnp.float32), 0.25, 1.75)
    weight_bias = centred(splits[15], (WIDTH,), 0.5, 3.0, ((0, 4),), jnp.float32)
    moment_up = centred(splits[16], (WIDTH, INNER), WIDTH ** -0.5, 0.1875, ((0, 4), (1, 8)), jnp.float32)
    moment_down = centred(splits[17], (INNER, WIDTH), INNER ** -0.5, 0.09375, ((0, 8), (1, 4)), jnp.float32)
    moment_query = centred(splits[18], (WIDTH, ATTN), WIDTH ** -0.5, 0.1875, ((0, 4), (1, 8)), jnp.float32)
    moment_key = centred(splits[19], (WIDTH, ATTN), WIDTH ** -0.5, 0.1875, ((0, 4), (1, 8)), jnp.float32)
    moment_value = centred(splits[20], (WIDTH, ATTN), WIDTH ** -0.5, 0.1875, ((0, 4), (1, 8)), jnp.float32)
    moment_mixed = centred(splits[21], (ATTN, WIDTH), ATTN ** -0.5, 0.1875, ((0, 8), (1, 4)), jnp.float32)
    moment_norm = centred(splits[22], (WIDTH,), 0.3, 1.75, ((0, 4),), jnp.float32)
    moment_bias = centred(splits[23], (WIDTH,), 0.3, 1.75, ((0, 4),), jnp.float32)
    return dict(grad_up=grad_up, grad_down=grad_down, grad_query=grad_query, grad_key=grad_key, grad_value=grad_value, grad_mixed=grad_mixed, grad_norm=grad_norm, grad_bias=grad_bias, weight_up=weight_up, weight_down=weight_down, weight_query=weight_query, weight_key=weight_key, weight_value=weight_value, weight_mixed=weight_mixed, weight_norm=weight_norm, weight_bias=weight_bias, moment_up=moment_up, moment_down=moment_down, moment_query=moment_query, moment_key=moment_key, moment_value=moment_value, moment_mixed=moment_mixed, moment_norm=moment_norm, moment_bias=moment_bias)


learn_rate = 0.4
hold_rate = 0.9

def reference(grad_up, grad_down, grad_query, grad_key, grad_value, grad_mixed, grad_norm, grad_bias, weight_up, weight_down, weight_query, weight_key, weight_value, weight_mixed, weight_norm, weight_bias, moment_up, moment_down, moment_query, moment_key, moment_value, moment_mixed, moment_norm, moment_bias):
    mean_up = lax.optimization_barrier(jnp.sum(grad_up.astype(jnp.float32), axis=0)) * REPLICAS ** (-0.5)
    mean_down = lax.optimization_barrier(jnp.sum(grad_down.astype(jnp.float32), axis=0)) * REPLICAS ** (-0.5)
    mean_query = lax.optimization_barrier(jnp.sum(grad_query.astype(jnp.float32), axis=0)) * REPLICAS ** (-0.5)
    mean_key = lax.optimization_barrier(jnp.sum(grad_key.astype(jnp.float32), axis=0)) * REPLICAS ** (-0.5)
    mean_value = lax.optimization_barrier(jnp.sum(grad_value.astype(jnp.float32), axis=0)) * REPLICAS ** (-0.5)
    mean_mixed = lax.optimization_barrier(jnp.sum(grad_mixed.astype(jnp.float32), axis=0)) * REPLICAS ** (-0.5)
    mean_norm = lax.optimization_barrier(jnp.sum(grad_norm.astype(jnp.float32), axis=0)) * REPLICAS ** (-0.5)
    mean_bias = lax.optimization_barrier(jnp.sum(grad_bias.astype(jnp.float32), axis=0)) * REPLICAS ** (-0.5)
    ratio_up = jnp.sqrt(lax.optimization_barrier(jnp.sum(weight_up * weight_up, axis=1, keepdims=True))) * lax.rsqrt(lax.optimization_barrier(jnp.sum(mean_up * mean_up, axis=1, keepdims=True)) + 1e-06)
    mean_up = mean_up * ratio_up
    ratio_down = jnp.sqrt(lax.optimization_barrier(jnp.sum(weight_down * weight_down, axis=0, keepdims=True))) * lax.rsqrt(lax.optimization_barrier(jnp.sum(mean_down * mean_down, axis=0, keepdims=True)) + 1e-06)
    mean_down = mean_down * ratio_down
    ratio_query = jnp.sqrt(lax.optimization_barrier(jnp.sum(weight_query * weight_query, axis=1, keepdims=True))) * lax.rsqrt(lax.optimization_barrier(jnp.sum(mean_query * mean_query, axis=1, keepdims=True)) + 1e-06)
    mean_query = mean_query * ratio_query
    ratio_key = jnp.sqrt(lax.optimization_barrier(jnp.sum(weight_key * weight_key, axis=1, keepdims=True))) * lax.rsqrt(lax.optimization_barrier(jnp.sum(mean_key * mean_key, axis=1, keepdims=True)) + 1e-06)
    mean_key = mean_key * ratio_key
    ratio_value = jnp.sqrt(lax.optimization_barrier(jnp.sum(weight_value * weight_value, axis=1, keepdims=True))) * lax.rsqrt(lax.optimization_barrier(jnp.sum(mean_value * mean_value, axis=1, keepdims=True)) + 1e-06)
    mean_value = mean_value * ratio_value
    ratio_mixed = jnp.sqrt(lax.optimization_barrier(jnp.sum(weight_mixed * weight_mixed, axis=0, keepdims=True))) * lax.rsqrt(lax.optimization_barrier(jnp.sum(mean_mixed * mean_mixed, axis=0, keepdims=True)) + 1e-06)
    mean_mixed = mean_mixed * ratio_mixed
    state_new_up = hold_rate * moment_up + mean_up
    new_up = weight_up - learn_rate * state_new_up
    state_new_down = hold_rate * moment_down + mean_down
    new_down = weight_down - learn_rate * state_new_down
    state_new_query = hold_rate * moment_query + mean_query
    new_query = weight_query - learn_rate * state_new_query
    state_new_key = hold_rate * moment_key + mean_key
    new_key = weight_key - learn_rate * state_new_key
    state_new_value = hold_rate * moment_value + mean_value
    new_value = weight_value - learn_rate * state_new_value
    state_new_mixed = hold_rate * moment_mixed + mean_mixed
    new_mixed = weight_mixed - learn_rate * state_new_mixed
    state_new_norm = hold_rate * moment_norm + mean_norm
    new_norm = weight_norm - learn_rate * state_new_norm
    state_new_bias = hold_rate * moment_bias + mean_bias
    new_bias = weight_bias - learn_rate * state_new_bias
    copy_up = new_up.astype(jnp.bfloat16)
    copy_down = new_down.astype(jnp.bfloat16)
    copy_query = new_query.astype(jnp.bfloat16)
    copy_key = new_key.astype(jnp.bfloat16)
    copy_value = new_value.astype(jnp.bfloat16)
    copy_mixed = new_mixed.astype(jnp.bfloat16)
    copy_norm = new_norm.astype(jnp.bfloat16)
    copy_bias = new_bias.astype(jnp.bfloat16)
    return (copy_up, copy_down, copy_query, copy_key, copy_value, copy_mixed, copy_norm, copy_bias, new_up, new_down, new_query, new_key, new_value, new_mixed, new_norm, new_bias, state_new_up, state_new_down, state_new_query, state_new_key, state_new_value, state_new_mixed, state_new_norm, state_new_bias)
```

```python
import functools

import jax
import jax.numpy as jnp
from jax import lax
from jax.experimental import pallas as pl
from jax.experimental.pallas import tpu as pltpu
from jax.sharding import PartitionSpec as P

learn_rate = 0.4
hold_rate = 0.9
tile = 128
matrices = ("up", "down", "query", "key", "value", "mixed")
by_rows = {"up": True, "down": False, "query": True, "key": True, "value": True, "mixed": False}
ahead = 2


class Piece:
    def __init__(self, at, rows_cut, share, start, size, other):
        self.at = at
        self.rows_cut = rows_cut
        self.share = share
        self.start = start
        self.size = size
        self.shape = (size, other) if rows_cut else (other, size)

    def tiles(self):
        r, c = self.shape
        h, w = min(tile, r), min(tile, c)
        return [(i, j, h, w) for i in range(0, r, h) for j in range(0, c, w)]

    def span(self, share, i, j, h, w):
        base = share * self.share
        if self.rows_cut:
            return pl.ds(aligned(base + (self.start + i), h), h), pl.ds(j, w)
        return pl.ds(i, h), pl.ds(aligned(base + (self.start + j), w), w)

    def own(self, i, j, h, w):
        if self.rows_cut:
            return pl.ds(self.start + i, h), pl.ds(j, w)
        return pl.ds(i, h), pl.ds(self.start + j, w)


def aligned(place, size):
    return place if isinstance(place, int) else pl.multiple_of(place, size)


def pieces_of(weights):
    def cut(at, parts=1):
        rows_cut = by_rows[matrices[at]]
        r, c = weights[at].shape
        share, other = (r, c) if rows_cut else (c, r)
        if share % (parts * tile):
            parts = 1
        size = share // parts
        return [Piece(at, rows_cut, share, k * size, size, other) for k in range(parts)]

    return cut(2) + cut(3) + cut(0, 2) + cut(1, 2) + cut(4) + cut(5)


def kernel(pieces, n, m, *refs):
    k = len(matrices)
    grads, weights, moments, vec_ref = refs[:k], refs[k : 2 * k], refs[2 * k : 3 * k], refs[3 * k]
    outs = refs[3 * k + 1 : 6 * k + 2]
    copies, news, states, vecs = outs[:k], outs[k : 2 * k], outs[2 * k : 3 * k], outs[3 * k]
    rest = refs[6 * k + 2 :]
    count = len(pieces)
    from_left, from_right = rest[:count], rest[count : 2 * count]
    totals, mine, theirs = rest[2 * count : 3 * count], rest[3 * count : 4 * count], rest[4 * count : 5 * count]
    (
        sent_right,
        sent_left,
        got_left,
        got_right,
        norm_sent,
        norm_got,
        copy_right,
        copy_left,
        copy_from_left,
        copy_from_right,
        vec_sent,
        vec_got,
    ) = rest[5 * count :]
    d = lax.axis_index("batch")
    e = lax.axis_index("cols")
    right, left = (lax.rem(d + 1, n), e), (lax.rem(d + n - 1, n), e)
    half = n // 2
    rate = n ** (-0.5)

    def send(src, dst, send_sem, recv_sem, where):
        return pltpu.make_async_remote_copy(
            src_ref=src,
            dst_ref=dst,
            send_sem=send_sem,
            recv_sem=recv_sem,
            device_id=where,
            device_id_type=pl.DeviceIdType.MESH,
        )

    barrier = pltpu.get_barrier_semaphore()
    for step in range(1, n):
        pl.semaphore_signal(
            barrier, inc=1, device_id=(lax.rem(d + step, n), e), device_id_type=pl.DeviceIdType.MESH
        )
    for step in range(1, m):
        pl.semaphore_signal(
            barrier, inc=1, device_id=(d, lax.rem(e + step, m)), device_id_type=pl.DeviceIdType.MESH
        )
    pl.semaphore_wait(barrier, n + m - 2)

    def hop(p, s, to_right, first):
        piece = pieces[p]
        buffer = (from_left if to_right else from_right)[p]
        sems = (sent_right, got_left) if to_right else (sent_left, got_right)
        if first:
            src = grads[piece.at].at[(0, *piece.span(s, 0, 0, *piece.shape))]
        else:
            src = buffer.at[s]
        where = right if to_right else left
        return send(src, buffer.at[s], sems[0].at[p, s], sems[1].at[p, s], where)

    def start_line(p):
        @pl.when(d == 0)
        def _():
            for s in reversed(range(1, n)):
                hop(p, s, True, True).start()

        @pl.when(d == n - 1)
        def _():
            for s in range(n - 1):
                hop(p, s, False, True).start()

    def relay(p, to_right, when):
        piece = pieces[p]
        buffer = (from_left if to_right else from_right)[p]
        inner = (d > 0) if to_right else (d < n - 1)
        for s in reversed(range(2, n)) if to_right else range(n - 2):
            beyond = (d < s) if to_right else (d > s)

            @pl.when(when & inner & beyond)
            def _():
                hop(p, s, to_right, False).wait_recv()
                for i, j, h, w in piece.tiles():
                    here = (s, pl.ds(i, h), pl.ds(j, w))
                    buffer[here] = buffer[here] + grads[piece.at][(0, *piece.span(s, i, j, h, w))]
                hop(p, s, to_right, False).start()

    def early(p):
        relay(p, True, d < half)
        relay(p, False, d >= half)

    def late(p):
        relay(p, False, d < half)
        relay(p, True, d >= half)

    def norm_copy(p, step):
        return send(
            mine[p],
            theirs[p].at[step - 1],
            norm_sent.at[p, step - 1],
            norm_got.at[p, step - 1],
            (d, lax.rem(e + step, m)),
        )

    def combine(p):
        piece = pieces[p]
        g, w_ref, total = grads[piece.at], weights[piece.at], totals[p]

        @pl.when(d > 0)
        def _():
            hop(p, d, True, False).wait_recv()

        @pl.when(d < n - 1)
        def _():
            hop(p, d, False, False).wait_recv()

        @pl.when(d == 0)
        def _():
            from_left[p][0] = jnp.zeros(piece.shape, jnp.float32)

        @pl.when(d == n - 1)
        def _():
            from_right[p][n - 1] = jnp.zeros(piece.shape, jnp.float32)

        mine[p][...] = jnp.zeros(mine[p].shape, jnp.float32)
        sums = {}
        for i, j, h, w in piece.tiles():
            here = (d, pl.ds(i, h), pl.ds(j, w))
            value = (from_left[p][here] + g[(0, *piece.span(d, i, j, h, w))]) + from_right[p][here]
            value = value * rate
            total[pl.ds(i, h), pl.ds(j, w)] = value
            weight = w_ref[piece.own(i, j, h, w)]
            pair = (weight * weight, value * value)
            if not piece.rows_cut:
                pair = tuple(jnp.sum(x, axis=0, keepdims=True) for x in pair)
            key = i if piece.rows_cut else j
            sums[key] = tuple(a + b for a, b in zip(sums[key], pair)) if key in sums else pair
        for key, pair in sums.items():
            if piece.rows_cut:
                pair = tuple(jnp.sum(x.T, axis=0, keepdims=True) for x in pair)
            for row, x in enumerate(pair):
                mine[p][pl.ds(row, 1), pl.ds(key, x.shape[1])] = x
        for step in range(1, m):
            norm_copy(p, step).start()

    def copy_block(p, owner):
        piece = pieces[p]
        return copies[piece.at].at[piece.span(owner, 0, 0, *piece.shape)]

    def copy_hop(p, k, to_right):
        owner = d - (k - 1) if to_right else d + (k - 1)
        sems = (copy_right, copy_from_left) if to_right else (copy_left, copy_from_right)
        where = right if to_right else left
        block = copy_block(p, owner)
        return send(block, block, sems[0].at[p, k - 1], sems[1].at[p, k - 1], where)

    def copy_wait(p, k, to_right):
        owner = d - k if to_right else d + k
        sems = (copy_right, copy_from_left) if to_right else (copy_left, copy_from_right)
        block = copy_block(p, owner)
        send(block, block, sems[0].at[p, k - 1], sems[1].at[p, k - 1], right).wait_recv()

    def update(p):
        piece = pieces[p]
        for step in range(1, m):
            norm_copy(p, step).wait_recv()
        squares = mine[p][...]
        for step in range(1, m):
            squares = squares + theirs[p][step - 1]
        ratio = jnp.sqrt(squares[0:1]) * lax.rsqrt(squares[1:2] + 1e-06)
        spread = {}
        for i, j, h, w in piece.tiles():
            key = i if piece.rows_cut else j
            if key not in spread:
                if piece.rows_cut:
                    spread[key] = jnp.broadcast_to(ratio[:, i : i + h], (w, h)).T
                else:
                    spread[key] = ratio[:, j : j + w]
            own = piece.own(i, j, h, w)
            mean = totals[p][pl.ds(i, h), pl.ds(j, w)] * spread[key]
            state = hold_rate * moments[piece.at][own] + mean
            new = weights[piece.at][own] - learn_rate * state
            states[piece.at][own] = state
            news[piece.at][own] = new
            copies[piece.at][piece.span(d, i, j, h, w)] = new.astype(jnp.bfloat16)
        hand_on(p, 1)

    def hand_on(p, k):
        @pl.when(d >= k - 1)
        def _():
            if k > 1:
                copy_wait(p, k - 1, True)
            if k < n:

                @pl.when(d < n - 1)
                def _():
                    copy_hop(p, k, True).start()

        @pl.when(d <= n - k)
        def _():
            if k > 1:
                copy_wait(p, k - 1, False)
            if k < n:

                @pl.when(d > 0)
                def _():
                    copy_hop(p, k, False).start()

    def vec_copy(step):
        return send(
            vec_ref,
            vecs.at[d],
            vec_sent.at[step - 1],
            vec_got.at[step - 1],
            (lax.rem(d + step, n), e),
        )

    def vec_from(step):
        source = lax.rem(d - step + n, n)
        return send(vec_ref, vecs.at[source], vec_sent.at[step - 1], vec_got.at[step - 1], (lax.rem(d + step, n), e))

    for p in range(min(ahead, count)):
        start_line(p)
        if p == 0:
            for step in range(1, n):
                vec_copy(step).start()
            vecs[d] = vec_ref[...]
    for t in range(count + 3 + n):
        stages = [(start_line, ahead), (early, 0), (late, -1), (combine, -2), (update, -3)]
        for stage, lag in stages:
            if 0 <= t + lag < count:
                stage(t + lag)
        for k in range(2, n + 1):
            if 0 <= t - 2 - k < count:
                hand_on(t - 2 - k, k)

    for step in range(1, n):
        vec_from(step).wait_recv()
        vec_copy(step).wait_send()
    for p in range(count):
        for s in range(1, n):

            @pl.when(d < s)
            def _():
                hop(p, s, True, False).wait_send()

        for s in range(n - 1):

            @pl.when(d > s)
            def _():
                hop(p, s, False, False).wait_send()

        for step in range(1, m):
            norm_copy(p, step).wait_send()
        for k in range(1, n):

            @pl.when((d >= k - 1) & (d < n - 1))
            def _():
                copy_hop(p, k, True).wait_send()

            @pl.when((d <= n - k) & (d > 0))
            def _():
                copy_hop(p, k, False).wait_send()


def local(*args):
    grads, weights, moments = args[:6], args[8:14], args[16:22]
    grad_vecs, weight_vecs, moment_vecs = args[6:8], args[14:16], args[22:24]
    n, m = lax.axis_size("batch"), lax.axis_size("cols")
    pieces = pieces_of(weights)
    count = len(pieces)
    width = grad_vecs[0].shape[1]
    part = weight_vecs[0].shape[0]

    shares = jnp.concatenate((*weight_vecs, *moment_vecs))
    shares = jnp.pad(shares, (0, width - shares.shape[0]))
    message = jnp.stack((grad_vecs[0][0], grad_vecs[1][0], shares))
    message = jnp.pad(message, ((0, 5), (0, 0)))

    f32 = jnp.float32
    out_shape = (
        [jax.ShapeDtypeStruct(g.shape[1:], jnp.bfloat16) for g in grads]
        + [jax.ShapeDtypeStruct(w.shape, f32) for w in weights] * 2
        + [jax.ShapeDtypeStruct((n, 8, width), f32)]
    )
    scratch = [pltpu.VMEM((n, *p.shape), f32) for p in pieces] * 2
    scratch += [pltpu.VMEM(p.shape, f32) for p in pieces]
    scratch += [pltpu.VMEM((8, max(tile, p.size)), f32) for p in pieces]
    scratch += [pltpu.VMEM((m - 1, 8, max(tile, p.size)), f32) for p in pieces]
    dma = pltpu.SemaphoreType.DMA
    scratch += [dma((count, n))] * 4 + [dma((count, m - 1))] * 2 + [dma((count, n - 1))] * 4
    scratch += [dma((n - 1,))] * 2
    vmem = pl.BlockSpec(memory_space=pltpu.VMEM)
    results = pl.pallas_call(
        functools.partial(kernel, pieces, n, m),
        out_shape=out_shape,
        in_specs=[vmem] * 19,
        out_specs=[vmem] * len(out_shape),
        scratch_shapes=scratch,
        compiler_params=pltpu.CompilerParams(
            collective_id=0, has_side_effects=True, vmem_limit_bytes=60 * 1024 * 1024
        ),
    )(*grads, *weights, *moments, message)
    copies, news, states, vecs = results[:6], results[6:12], results[12:18], results[18]

    whole = vecs[0, :2]
    for s in range(1, n):
        whole = whole + vecs[s, :2]
    mean = whole * n ** (-0.5)
    held = vecs[:, 2, : 4 * part].reshape(n, 2, 2, part).transpose(1, 2, 0, 3).reshape(2, 2, width)
    vec_copy = (held[0] - learn_rate * (hold_rate * held[1] + mean)).astype(jnp.bfloat16)
    place = lax.axis_index("batch")
    own_mean = lax.dynamic_slice_in_dim(mean, place * part, part, axis=1)
    vec_state = [hold_rate * moment_vecs[k] + own_mean[k] for k in range(2)]
    vec_new = [weight_vecs[k] - learn_rate * vec_state[k] for k in range(2)]
    return (*copies, vec_copy[0], vec_copy[1], *news, *vec_new, *states, *vec_state)


def solution(mesh):
    grads = [P("batch", None, "cols") if by_rows[x] else P("batch", "cols", None) for x in matrices]
    held = [P("batch", "cols") if by_rows[x] else P("cols", "batch") for x in matrices]
    whole = [P(None, "cols") if by_rows[x] else P("cols", None) for x in matrices]
    vector = [P("batch")] * 2
    return jax.shard_map(
        local,
        mesh=mesh,
        in_specs=(*grads, P("batch", None), P("batch", None), *held, *vector, *held, *vector),
        out_specs=(*whole, P(), P(), *held, *vector, *held, *vector),
        check_vma=False,
    )
```

```python
import functools

import jax
import jax.numpy as jnp
from jax import lax
from jax.experimental import pallas as pl
from jax.experimental.pallas import tpu as pltpu
from jax.sharding import PartitionSpec as P

learn_rate = 0.4
hold_rate = 0.9
tile = 128
matrices = ("up", "down", "query", "key", "value", "mixed")
by_rows = {"up": True, "down": False, "query": True, "key": True, "value": True, "mixed": False}
ahead = 2


class Piece:
    def __init__(self, at, rows_cut, share, start, size, other):
        self.at = at
        self.rows_cut = rows_cut
        self.share = share
        self.start = start
        self.size = size
        self.shape = (size, other) if rows_cut else (other, size)

    def tiles(self):
        r, c = self.shape
        h, w = min(tile, r), min(tile, c)
        return [(i, j, h, w) for i in range(0, r, h) for j in range(0, c, w)]

    def span(self, share, i, j, h, w):
        base = share * self.share
        if self.rows_cut:
            return pl.ds(aligned(base + (self.start + i), h), h), pl.ds(j, w)
        return pl.ds(i, h), pl.ds(aligned(base + (self.start + j), w), w)

    def own(self, i, j, h, w):
        if self.rows_cut:
            return pl.ds(self.start + i, h), pl.ds(j, w)
        return pl.ds(i, h), pl.ds(self.start + j, w)


def aligned(place, size):
    return place if isinstance(place, int) else pl.multiple_of(place, size)


def pieces_of(weights):
    def cut(at, parts=1):
        rows_cut = by_rows[matrices[at]]
        r, c = weights[at].shape
        share, other = (r, c) if rows_cut else (c, r)
        if share % (parts * tile):
            parts = 1
        size = share // parts
        return [Piece(at, rows_cut, share, k * size, size, other) for k in range(parts)]

    return cut(2) + cut(3) + cut(0, 2) + cut(1, 2) + cut(4) + cut(5)


def kernel(pieces, n, m, *refs):
    k = len(matrices)
    grads, weights, moments, vec_ref = refs[:k], refs[k : 2 * k], refs[2 * k : 3 * k], refs[3 * k]
    outs = refs[3 * k + 1 : 5 * k + 2]
    copies, means, vecs = outs[:k], outs[k : 2 * k], outs[2 * k]
    rest = refs[5 * k + 2 :]
    count = len(pieces)
    from_left, from_right = rest[:count], rest[count : 2 * count]
    totals, mine, theirs = rest[2 * count : 3 * count], rest[3 * count : 4 * count], rest[4 * count : 5 * count]
    (
        sent_right,
        sent_left,
        got_left,
        got_right,
        norm_sent,
        norm_got,
        copy_right,
        copy_left,
        copy_from_left,
        copy_from_right,
        vec_sent,
        vec_got,
    ) = rest[5 * count :]
    d = lax.axis_index("batch")
    e = lax.axis_index("cols")
    right, left = (lax.rem(d + 1, n), e), (lax.rem(d + n - 1, n), e)
    half = n // 2
    rate = n ** (-0.5)

    def send(src, dst, send_sem, recv_sem, where):
        return pltpu.make_async_remote_copy(
            src_ref=src,
            dst_ref=dst,
            send_sem=send_sem,
            recv_sem=recv_sem,
            device_id=where,
            device_id_type=pl.DeviceIdType.MESH,
        )

    barrier = pltpu.get_barrier_semaphore()
    for step in range(1, n):
        pl.semaphore_signal(
            barrier, inc=1, device_id=(lax.rem(d + step, n), e), device_id_type=pl.DeviceIdType.MESH
        )
    for step in range(1, m):
        pl.semaphore_signal(
            barrier, inc=1, device_id=(d, lax.rem(e + step, m)), device_id_type=pl.DeviceIdType.MESH
        )
    pl.semaphore_wait(barrier, n + m - 2)

    def hop(p, s, to_right, first):
        piece = pieces[p]
        buffer = (from_left if to_right else from_right)[p]
        sems = (sent_right, got_left) if to_right else (sent_left, got_right)
        if first:
            src = grads[piece.at].at[(0, *piece.span(s, 0, 0, *piece.shape))]
        else:
            src = buffer.at[s]
        where = right if to_right else left
        return send(src, buffer.at[s], sems[0].at[p, s], sems[1].at[p, s], where)

    def start_line(p):
        @pl.when(d == 0)
        def _():
            for s in reversed(range(1, n)):
                hop(p, s, True, True).start()

        @pl.when(d == n - 1)
        def _():
            for s in range(n - 1):
                hop(p, s, False, True).start()

    def relay(p, to_right, when):
        piece = pieces[p]
        buffer = (from_left if to_right else from_right)[p]
        inner = (d > 0) if to_right else (d < n - 1)
        for s in reversed(range(2, n)) if to_right else range(n - 2):
            beyond = (d < s) if to_right else (d > s)

            @pl.when(when & inner & beyond)
            def _():
                hop(p, s, to_right, False).wait_recv()
                for i, j, h, w in piece.tiles():
                    here = (s, pl.ds(i, h), pl.ds(j, w))
                    buffer[here] = buffer[here] + grads[piece.at][(0, *piece.span(s, i, j, h, w))]
                hop(p, s, to_right, False).start()

    def early(p):
        relay(p, True, d < half)
        relay(p, False, d >= half)

    def late(p):
        relay(p, False, d < half)
        relay(p, True, d >= half)

    def norm_copy(p, step):
        return send(
            mine[p],
            theirs[p].at[step - 1],
            norm_sent.at[p, step - 1],
            norm_got.at[p, step - 1],
            (d, lax.rem(e + step, m)),
        )

    def combine(p):
        piece = pieces[p]
        g, w_ref, total = grads[piece.at], weights[piece.at], totals[p]

        @pl.when(d > 0)
        def _():
            hop(p, d, True, False).wait_recv()

        @pl.when(d < n - 1)
        def _():
            hop(p, d, False, False).wait_recv()

        @pl.when(d == 0)
        def _():
            from_left[p][0] = jnp.zeros(piece.shape, jnp.float32)

        @pl.when(d == n - 1)
        def _():
            from_right[p][n - 1] = jnp.zeros(piece.shape, jnp.float32)

        mine[p][...] = jnp.zeros(mine[p].shape, jnp.float32)
        sums = {}
        for i, j, h, w in piece.tiles():
            here = (d, pl.ds(i, h), pl.ds(j, w))
            value = (from_left[p][here] + g[(0, *piece.span(d, i, j, h, w))]) + from_right[p][here]
            value = value * rate
            total[pl.ds(i, h), pl.ds(j, w)] = value
            weight = w_ref[piece.own(i, j, h, w)]
            pair = (weight * weight, value * value)
            if not piece.rows_cut:
                pair = tuple(jnp.sum(x, axis=0, keepdims=True) for x in pair)
            key = i if piece.rows_cut else j
            sums[key] = tuple(a + b for a, b in zip(sums[key], pair)) if key in sums else pair
        for key, pair in sums.items():
            if piece.rows_cut:
                pair = tuple(jnp.sum(x.T, axis=0, keepdims=True) for x in pair)
            for row, x in enumerate(pair):
                mine[p][pl.ds(row, 1), pl.ds(key, x.shape[1])] = x
        for step in range(1, m):
            norm_copy(p, step).start()

    def copy_block(p, owner):
        piece = pieces[p]
        return copies[piece.at].at[piece.span(owner, 0, 0, *piece.shape)]

    def copy_hop(p, k, to_right):
        owner = d - (k - 1) if to_right else d + (k - 1)
        sems = (copy_right, copy_from_left) if to_right else (copy_left, copy_from_right)
        where = right if to_right else left
        block = copy_block(p, owner)
        return send(block, block, sems[0].at[p, k - 1], sems[1].at[p, k - 1], where)

    def copy_wait(p, k, to_right):
        owner = d - k if to_right else d + k
        sems = (copy_right, copy_from_left) if to_right else (copy_left, copy_from_right)
        block = copy_block(p, owner)
        send(block, block, sems[0].at[p, k - 1], sems[1].at[p, k - 1], right).wait_recv()

    def update(p):
        piece = pieces[p]
        for step in range(1, m):
            norm_copy(p, step).wait_recv()
        squares = mine[p][...]
        for step in range(1, m):
            squares = squares + theirs[p][step - 1]
        ratio = jnp.sqrt(squares[0:1]) * lax.rsqrt(squares[1:2] + 1e-06)
        spread = {}
        for i, j, h, w in piece.tiles():
            key = i if piece.rows_cut else j
            if key not in spread:
                if piece.rows_cut:
                    spread[key] = jnp.broadcast_to(ratio[:, i : i + h], (w, h)).T
                else:
                    spread[key] = ratio[:, j : j + w]
            own = piece.own(i, j, h, w)
            mean = totals[p][pl.ds(i, h), pl.ds(j, w)] * spread[key]
            state = hold_rate * moments[piece.at][own] + mean
            new = weights[piece.at][own] - learn_rate * state
            means[piece.at][own] = mean
            copies[piece.at][piece.span(d, i, j, h, w)] = new.astype(jnp.bfloat16)
        hand_on(p, 1)

    def hand_on(p, k):
        @pl.when(d >= k - 1)
        def _():
            if k > 1:
                copy_wait(p, k - 1, True)
            if k < n:

                @pl.when(d < n - 1)
                def _():
                    copy_hop(p, k, True).start()

        @pl.when(d <= n - k)
        def _():
            if k > 1:
                copy_wait(p, k - 1, False)
            if k < n:

                @pl.when(d > 0)
                def _():
                    copy_hop(p, k, False).start()

    def vec_copy(step):
        return send(
            vec_ref,
            vecs.at[d],
            vec_sent.at[step - 1],
            vec_got.at[step - 1],
            (lax.rem(d + step, n), e),
        )

    def vec_from(step):
        source = lax.rem(d - step + n, n)
        return send(vec_ref, vecs.at[source], vec_sent.at[step - 1], vec_got.at[step - 1], (lax.rem(d + step, n), e))

    for p in range(min(ahead, count)):
        start_line(p)
        if p == 0:
            for step in range(1, n):
                vec_copy(step).start()
            vecs[d] = vec_ref[...]
    for t in range(count + 3 + n):
        stages = [(start_line, ahead), (early, 0), (late, -1), (combine, -2), (update, -3)]
        for stage, lag in stages:
            if 0 <= t + lag < count:
                stage(t + lag)
        for k in range(2, n + 1):
            if 0 <= t - 3 - k < count:
                hand_on(t - 3 - k, k)

    for step in range(1, n):
        vec_from(step).wait_recv()
        vec_copy(step).wait_send()
    for p in range(count):
        for s in range(1, n):

            @pl.when(d < s)
            def _():
                hop(p, s, True, False).wait_send()

        for s in range(n - 1):

            @pl.when(d > s)
            def _():
                hop(p, s, False, False).wait_send()

        for step in range(1, m):
            norm_copy(p, step).wait_send()
        for k in range(1, n):

            @pl.when((d >= k - 1) & (d < n - 1))
            def _():
                copy_hop(p, k, True).wait_send()

            @pl.when((d <= n - k) & (d > 0))
            def _():
                copy_hop(p, k, False).wait_send()


def local(*args):
    grads, weights, moments = args[:6], args[8:14], args[16:22]
    grad_vecs, weight_vecs, moment_vecs = args[6:8], args[14:16], args[22:24]
    n, m = lax.axis_size("batch"), lax.axis_size("cols")
    pieces = pieces_of(weights)
    count = len(pieces)
    width = grad_vecs[0].shape[1]
    part = weight_vecs[0].shape[0]

    shares = jnp.concatenate((*weight_vecs, *moment_vecs))
    shares = jnp.pad(shares, (0, width - shares.shape[0]))
    message = jnp.stack((grad_vecs[0][0], grad_vecs[1][0], shares))
    message = jnp.pad(message, ((0, 5), (0, 0)))

    f32 = jnp.float32
    out_shape = (
        [jax.ShapeDtypeStruct(g.shape[1:], jnp.bfloat16) for g in grads]
        + [jax.ShapeDtypeStruct(w.shape, f32) for w in weights]
        + [jax.ShapeDtypeStruct((n, 8, width), f32)]
    )
    scratch = [pltpu.VMEM((n, *p.shape), f32) for p in pieces] * 2
    scratch += [pltpu.VMEM(p.shape, f32) for p in pieces]
    scratch += [pltpu.VMEM((8, max(tile, p.size)), f32) for p in pieces]
    scratch += [pltpu.VMEM((m - 1, 8, max(tile, p.size)), f32) for p in pieces]
    dma = pltpu.SemaphoreType.DMA
    scratch += [dma((count, n))] * 4 + [dma((count, m - 1))] * 2 + [dma((count, n - 1))] * 4
    scratch += [dma((n - 1,))] * 2
    vmem = pl.BlockSpec(memory_space=pltpu.VMEM)
    results = pl.pallas_call(
        functools.partial(kernel, pieces, n, m),
        out_shape=out_shape,
        in_specs=[vmem] * 19,
        out_specs=[vmem] * len(out_shape),
        scratch_shapes=scratch,
        compiler_params=pltpu.CompilerParams(
            collective_id=0, has_side_effects=True, vmem_limit_bytes=60 * 1024 * 1024
        ),
    )(*grads, *weights, *moments, message)
    copies, means, vecs = results[:6], results[6:12], results[12]
    states = [hold_rate * x + mean for x, mean in zip(moments, means)]
    news = [x - learn_rate * state for x, state in zip(weights, states)]

    whole = vecs[0, :2]
    for s in range(1, n):
        whole = whole + vecs[s, :2]
    mean = whole * n ** (-0.5)
    held = vecs[:, 2, : 4 * part].reshape(n, 2, 2, part).transpose(1, 2, 0, 3).reshape(2, 2, width)
    vec_copy = (held[0] - learn_rate * (hold_rate * held[1] + mean)).astype(jnp.bfloat16)
    place = lax.axis_index("batch")
    own_mean = lax.dynamic_slice_in_dim(mean, place * part, part, axis=1)
    vec_state = [hold_rate * moment_vecs[k] + own_mean[k] for k in range(2)]
    vec_new = [weight_vecs[k] - learn_rate * vec_state[k] for k in range(2)]
    return (*copies, vec_copy[0], vec_copy[1], *news, *vec_new, *states, *vec_state)


def solution(mesh):
    grads = [P("batch", None, "cols") if by_rows[x] else P("batch", "cols", None) for x in matrices]
    held = [P("batch", "cols") if by_rows[x] else P("cols", "batch") for x in matrices]
    whole = [P(None, "cols") if by_rows[x] else P("cols", None) for x in matrices]
    vector = [P("batch")] * 2
    return jax.shard_map(
        local,
        mesh=mesh,
        in_specs=(*grads, P("batch", None), P("batch", None), *held, *vector, *held, *vector),
        out_specs=(*whole, P(), P(), *held, *vector, *held, *vector),
        check_vma=False,
    )
```
